512 devices in a mesh: inst: 64 (over z, x, core), tp: 8 (over y).
Axes of the slice: x: 4, y: 8, z: 8, core: 2. Of those that a mesh axis runs over, the one named last changes fastest.
Arguments:
- queries: bfloat16 [64, 4096], P('inst', 'tp'), may hold values from -360 to 360
- slot_request: int32 [64], P('inst'), may hold values from -1 to 31, as said below
- key_cache_pages: bfloat16 [2048, 128, 1024], P('inst', None, 'tp'), may hold values from -6 to 6
- value_cache_pages: bfloat16 [2048, 128, 1024], P('inst', None, 'tp'), may hold values from -6 to 6
- page_owner: int32 [2048], P('inst'), may hold values from -1 to 31, as said below
- page_fill: int32 [2048], P('inst'), may hold values from 1 to 128
- out_weight: bfloat16 [4096, 4096], P('tp', 'inst'), may hold values from -0.09375 to 0.09375
Outputs:
- projected: bfloat16 [64, 4096], P('inst', 'tp')
The draws below stay inside these ranges and needn't reach their ends.
Inputs may be any that keep to these rules, and one draw needn't show every extreme that they name: `slot_request`: each request id appears in exactly one slot; every other slot holds -1. `page_owner`: each entry is -1 (a free page) or a request id; every request owns at least one page.
All inputs are finite; a program needn't handle non-finite values.
Results may differ from the reference program's by a relative error of at most 0.005.
Values may be sent and summed in bfloat16 or wider, within the bound.
No kernel may reach another device: no remote copies, remote signals or barrier semaphores. Data moves between devices by JAX's collectives and lax.ppermute only.
A program may use at most 64 MiB of HBM per device.

```python
import math
import jax
import jax.numpy as jnp
from jax import lax

D = 4096
QUERY_HEADS = 32
KEY_VALUE_HEADS = 8
HEAD_SIZE = 128
PAGE_SLOTS = 128
LOCAL_PAGES = 32
SLOTS = 64
REQ = 32
ALL_PAGES = 2048
N_INST = 64


def draw_queries(key, part):
    base_key, scale_key = jax.random.split(jax.random.fold_in(key, 11))
    values = jnp.clip(jax.random.normal(base_key, (SLOTS, QUERY_HEADS, HEAD_SIZE), jnp.float32), -6.0, 6.0)
    row_scale = jnp.exp(jax.random.uniform(scale_key, (SLOTS, QUERY_HEADS, 1), jnp.float32, 0.0, math.log(4.0)))
    return (values * row_scale).reshape(SLOTS, QUERY_HEADS * HEAD_SIZE).astype(jnp.bfloat16)


def draw_slot_request(key, part):
    shuffled = jax.random.permutation(jax.random.fold_in(key, 31), SLOTS).astype(jnp.int32)
    return jnp.where(shuffled < REQ, shuffled, -1).astype(jnp.int32)


def draw_page_owner(key, part):
    start_key, size_key, score_key, free_key = jax.random.split(jax.random.fold_in(key, 23), 4)
    starts = jax.random.permutation(start_key, N_INST)[:REQ].astype(jnp.int32)
    widest = min(16, N_INST)
    group_size = jax.random.randint(size_key, (REQ,), 2, widest + 1).astype(jnp.int32)
    instance_ids = jnp.arange(N_INST, dtype=jnp.int32)
    offset = (instance_ids[:, None] - starts[None, :]) % N_INST
    covers = offset < group_size[None, :]
    request_ids = jnp.arange(REQ, dtype=jnp.int32)
    raw = jax.random.randint(score_key, (N_INST, LOCAL_PAGES, REQ), 0, 1 << 16).astype(jnp.int32)
    scores = raw * REQ + request_ids[None, None, :]
    scores = jnp.where(covers[:, None, :], scores, -1)
    best = jnp.argmax(scores, axis=-1).astype(jnp.int32)
    anyone = jnp.max(scores, axis=-1) >= 0
    is_free = jax.random.randint(free_key, (N_INST, LOCAL_PAGES), 0, 100) < 15
    owner_ids = jnp.where(anyone & jnp.logical_not(is_free), best, -1).astype(jnp.int32)
    is_start = instance_ids[:, None] == starts[None, :]
    start_owner = jnp.sum(jnp.where(is_start, request_ids[None, :] + 1, 0), axis=1).astype(jnp.int32) - 1
    first_page = jnp.where(start_owner >= 0, start_owner, owner_ids[:, 0])
    owner_ids = owner_ids.at[:, 0].set(first_page)
    return owner_ids.reshape(N_INST * LOCAL_PAGES).astype(jnp.int32)


def place_ends(entries, key, smallest, high):
    spot = [jax.random.randint(jax.random.fold_in(key, axis), (), 0, length) for axis, length in enumerate(entries.shape)]
    main_axis = entries.shape.index(max(entries.shape))
    neighbour = spot[:main_axis] + [(spot[main_axis] + 1) % entries.shape[main_axis]] + spot[main_axis + 1:]
    return entries.at[tuple(spot)].set(smallest).at[tuple(neighbour)].set(high)


def block_scale(own_key, extent, shards, low, largest):
    level = 1.0
    for dim, parts in shards:
        steps = jax.random.uniform(jax.random.fold_in(jax.random.fold_in(own_key, 6), dim), (parts,), jnp.float32, low / len(shards), largest / len(shards))
        level = level * jnp.repeat(jnp.exp(steps), extent[dim] // parts).reshape((-1,) + (1,) * (len(extent) - 1 - dim))
    return level


def noise(stream_key, dims, spread, reach, cuts=(), kind=jnp.bfloat16):
    drawn = jax.random.normal(stream_key, dims, jnp.float32) * spread
    if len(cuts) > 0:
        drawn = block_scale(stream_key, dims, cuts, -0.22, 0.18) * drawn
    return jnp.clip(drawn, min=-reach, max=reach).astype(kind)


def setup_inputs(seed: int = 0) -> dict:
    key_of = jax.random.split(jax.random.key(seed), 8)
    queries = draw_queries(jax.random.fold_in(key_of[7], 71), 0)
    slot_request = draw_slot_request(jax.random.fold_in(key_of[7], 71), 0)
    key_cache_pages = noise(key_of[2], (ALL_PAGES, PAGE_SLOTS, KEY_VALUE_HEADS * HEAD_SIZE), 1.0, 6.0, ((0, 64), (2, 8)))
    value_cache_pages = noise(key_of[3], (ALL_PAGES, PAGE_SLOTS, KEY_VALUE_HEADS * HEAD_SIZE), 1.0, 6.0, ((0, 64), (2, 8)))
    page_owner = draw_page_owner(jax.random.fold_in(key_of[7], 71), 0)
    page_fill = place_ends(jax.random.randint(key_of[5], (ALL_PAGES,), 1, PAGE_SLOTS + 1), jax.random.fold_in(key_of[5], 1), 1, PAGE_SLOTS).astype(jnp.int32)
    out_weight = noise(key_of[6], (QUERY_HEADS * HEAD_SIZE, D), (QUERY_HEADS * HEAD_SIZE) ** -0.5, 0.09375, ((0, 8), (1, 64)))
    return dict(queries=queries, slot_request=slot_request, key_cache_pages=key_cache_pages, value_cache_pages=value_cache_pages, page_owner=page_owner, page_fill=page_fill, out_weight=out_weight)


NEG_FILL = -1e30


def page_partials(by_request, block_of_keys, block_of_values, owner_block, fill_block):
    token_count = owner_block.shape[0]
    query_group = QUERY_HEADS // KEY_VALUE_HEADS
    selected_pages = by_request[jnp.clip(owner_block, 0, REQ - 1)]
    query_portion = selected_pages.reshape(token_count, KEY_VALUE_HEADS, query_group, HEAD_SIZE).astype(jnp.float32)
    key_portion = block_of_keys.reshape(token_count, PAGE_SLOTS, KEY_VALUE_HEADS, HEAD_SIZE).astype(jnp.float32)
    value_portion = block_of_values.reshape(token_count, PAGE_SLOTS, KEY_VALUE_HEADS, HEAD_SIZE).astype(jnp.float32)
    scores = jnp.einsum("bkgd,btkd->bkgt", query_portion, key_portion, precision=lax.Precision.HIGHEST) * (HEAD_SIZE ** -0.5)
    positions = jnp.arange(PAGE_SLOTS, dtype=jnp.int32)
    is_valid = positions[None, None, None, :] < fill_block[:, None, None, None]
    scores = jnp.where(is_valid, scores, NEG_FILL)
    page_peak = jnp.max(scores, axis=-1)
    expo_vals = jnp.exp(scores - page_peak[..., None])
    page_total = jnp.sum(expo_vals, axis=-1)
    prob_bf = lax.optimization_barrier(expo_vals.astype(jnp.bfloat16)).astype(jnp.float32)
    page_out = jnp.einsum("bkgt,btkd->bkgd", prob_bf, value_portion, precision=lax.Precision.HIGHEST)
    return page_out.reshape(token_count, QUERY_HEADS, HEAD_SIZE), page_peak.reshape(token_count, QUERY_HEADS), page_total.reshape(token_count, QUERY_HEADS)


def reference(queries, slot_request, key_cache_pages, value_cache_pages, page_owner, page_fill, out_weight):
    request_ids = jnp.arange(REQ, dtype=jnp.int32)
    slot_ids = jnp.arange(SLOTS, dtype=jnp.int32)
    matches = (slot_request[None, :] == request_ids[:, None]).astype(jnp.int32)
    slot_of = jnp.sum(matches * slot_ids[None, :], axis=1).astype(jnp.int32)
    by_request = queries[slot_of]

    def per_instance(block):
        return page_partials(by_request, block[0], block[1], block[2], block[3])

    reshaped_rows = (key_cache_pages.reshape(N_INST, LOCAL_PAGES, PAGE_SLOTS, KEY_VALUE_HEADS * HEAD_SIZE),
              value_cache_pages.reshape(N_INST, LOCAL_PAGES, PAGE_SLOTS, KEY_VALUE_HEADS * HEAD_SIZE),
              page_owner.reshape(N_INST, LOCAL_PAGES),
              page_fill.reshape(N_INST, LOCAL_PAGES))
    page_out, page_peak, page_total = lax.map(per_instance, reshaped_rows)
    page_out = page_out.reshape(N_INST * LOCAL_PAGES, QUERY_HEADS, HEAD_SIZE)
    page_peak = page_peak.reshape(N_INST * LOCAL_PAGES, QUERY_HEADS)
    page_total = page_total.reshape(N_INST * LOCAL_PAGES, QUERY_HEADS)
    segment = jnp.where(page_owner >= 0, page_owner, REQ).astype(jnp.int32)
    req_peak = jax.ops.segment_max(page_peak, segment, num_segments=REQ + 1)
    weight = jnp.exp(page_peak - req_peak[segment])
    req_total = jax.ops.segment_sum(weight * page_total, segment, num_segments=REQ + 1)[:REQ]
    req_out = jax.ops.segment_sum(weight[..., None] * page_out, segment, num_segments=REQ + 1)[:REQ]
    per_request = (req_out / req_total[..., None]).reshape(REQ, QUERY_HEADS * HEAD_SIZE)
    gathered = per_request[jnp.clip(slot_request, 0, REQ - 1).astype(jnp.int32)]
    attention = jnp.where((slot_request >= 0)[:, None], gathered, 0.0).astype(jnp.bfloat16)
    return jnp.dot(attention, out_weight, preferred_element_type=jnp.float32).astype(jnp.bfloat16)
```

```python
import functools

import jax
import jax.numpy as jnp
from jax import lax
from jax.experimental import pallas as pl
from jax.experimental.pallas import tpu as pltpu
from jax.sharding import Mesh, PartitionSpec as P

HEAD = 128
NEG_FILL = -1e30
F32, BF16 = jnp.float32, jnp.bfloat16
NT = (((1,), (1,)), ((), ()))
VMEM = pl.BlockSpec(memory_space=pltpu.VMEM)
SMEM = pl.BlockSpec(memory_space=pltpu.SMEM)


def iota(shape, dim):
    return lax.broadcasted_iota(jnp.int32, shape, dim)


def prepare(req_ref, q_ref, w_ref, out_ref):
    feats, cols = w_ref.shape
    eye = (iota((cols, cols), 0) == iota((cols, cols), 1)).astype(F32).astype(BF16)
    turned = lax.dot_general(eye, w_ref[...], NT, preferred_element_type=F32)
    half = cols // 2
    lane = iota((half, HEAD), 1)
    chunks = []
    for m in range(feats // HEAD):
        low = turned[:half, m * HEAD : (m + 1) * HEAD]
        high = turned[half:, m * HEAD : (m + 1) * HEAD]
        chunks.append(jnp.where(lane < 64, low, pltpu.roll(high, 64, 1)).astype(BF16))
        chunks.append(jnp.where(lane < 64, pltpu.roll(low, 64, 1), high).astype(BF16))
    row = iota((8, HEAD), 0)
    tile = jnp.full((8, HEAD), req_ref[0].astype(F32), F32)
    for h in range(4):
        head = q_ref[:, h * HEAD : (h + 1) * HEAD].astype(F32)
        tile = jnp.where(row == h, jnp.broadcast_to(head, (8, HEAD)), tile)
    tile = tile.astype(BF16)
    for d in range(out_ref.shape[0]):
        out_ref[d, 0:half, :] = chunks[d % len(chunks)]
        out_ref[d, half : half + 8, :] = tile


def three_parts(x):
    hi = x.astype(BF16).astype(F32)
    rest = x - hi
    mid = rest.astype(BF16).astype(F32)
    return hi, mid, rest - mid


def attend(owner_ref, fill_ref, got_ref, k_ref, v_ref, out_ref, peak_ref, mix_ref, sum_ref):
    n_slots = got_ref.shape[0]
    n_pages = k_ref.shape[0]
    n_req = peak_ref.shape[0] - 1
    rows = got_ref[:, 32:40, :].astype(F32).reshape(n_slots * 8, HEAD)
    rows_bf = rows.astype(BF16)
    first = (iota((8, HEAD), 1) == 0).astype(F32).astype(BF16)
    ids = lax.dot_general(first, rows_bf, NT, preferred_element_type=F32)
    blocks = [
        pltpu.roll(ids[:, b * HEAD : (b + 1) * HEAD], HEAD - 4, 1) for b in range(n_slots * 8 // HEAD)
    ]
    here = (iota((8, HEAD), 1) % 8 == iota((8, HEAD), 0)) & (iota((8, HEAD), 0) < 4)
    blocks = [jnp.where(here, b, -5.0) for b in blocks]
    owners = [owner_ref[p] for p in range(n_pages)]
    picks = []
    for p in range(n_pages):
        wanted = jnp.where(owners[p] >= 0, owners[p], -7).astype(F32)
        picks.append(jnp.concatenate([jnp.where(b == wanted, 1.0, 0.0) for b in blocks], axis=1))
    pick = jnp.concatenate(picks, axis=0).astype(BF16)
    page_q = jnp.dot(pick, rows_bf, preferred_element_type=F32)

    peak_ref[...] = jnp.full(peak_ref.shape, NEG_FILL, F32)
    mix_ref[...] = jnp.zeros(mix_ref.shape, F32)
    sum_ref[...] = jnp.zeros(sum_ref.shape, F32)
    token = iota((8, HEAD), 1)
    peaks, totals, outs = [], [], []
    for p in range(n_pages):
        score = lax.dot_general(
            page_q[p * 8 : (p + 1) * 8].astype(BF16), k_ref[p], NT, preferred_element_type=F32
        ) * (HEAD**-0.5)
        score = jnp.where(token < fill_ref[p], score, NEG_FILL)
        peak = jnp.max(score, axis=1, keepdims=True)
        e = jnp.exp(score - peak)
        totals.append(jnp.sum(e, axis=1, keepdims=True))
        outs.append(jnp.dot(e.astype(BF16), v_ref[p], preferred_element_type=F32))
        peaks.append(jnp.broadcast_to(peak, (8, HEAD)))
    index = [jnp.where(o >= 0, o, n_req) for o in owners]
    for p in range(n_pages):
        peak_ref[index[p]] = jnp.maximum(peak_ref[index[p]], peaks[p])
    for p in range(n_pages):
        weight = jnp.exp(peaks[p] - peak_ref[index[p]])
        mix_ref[index[p]] += weight * outs[p]
        sum_ref[index[p]] += weight * totals[p]

    n_rows = n_req * 8
    lane = iota((n_rows, HEAD), 1)
    mix = mix_ref[0:n_req].reshape(n_rows, HEAD)
    total = sum_ref[0:n_req].reshape(n_rows, HEAD)
    hi, mid, low = three_parts(peak_ref[0:n_req].reshape(n_rows, HEAD))
    total_hi = total.astype(BF16).astype(F32)
    stats = jnp.where(
        lane < 80,
        hi,
        jnp.where(lane < 96, mid, jnp.where(lane < 112, low, jnp.where(lane < 120, total_hi, total - total_hi))),
    )
    data = jnp.concatenate([mix.astype(BF16), stats.astype(BF16)], axis=1)
    place = (iota((n_slots, n_slots * 8), 1) == iota((n_slots, n_slots * 8), 0) * 8 + 4)
    slot_id = jnp.dot(place.astype(F32).astype(BF16), rows_bf, preferred_element_type=F32)[:, 0:1]
    col = iota((n_slots, n_rows), 1)
    owns = slot_id == (col // 8).astype(F32)
    lane8 = iota((n_slots, HEAD), 1)
    for h in range(4):
        chosen = jnp.where(owns & (col % 8 == h), 1.0, 0.0).astype(BF16)
        picked = jnp.dot(chosen, data, preferred_element_type=F32)
        o, st = picked[:, :HEAD], picked[:, HEAD:]
        left = jnp.where(lane8 < 64, o, st)
        right = jnp.where(lane8 < 64, pltpu.roll(o, 64, 1), st)
        for z in range(n_slots // 8):
            out_ref[z * 8 + 2 * h] = left[z * 8 : (z + 1) * 8].astype(BF16)
            out_ref[z * 8 + 2 * h + 1] = right[z * 8 : (z + 1) * 8].astype(BF16)


def project(part_ref, got_ref, out_ref):
    n_src = part_ref.shape[0]
    flat = part_ref[...].astype(F32).reshape(n_src * 8, HEAD)
    src = iota((HEAD, 2 * HEAD), 0)
    dst = iota((HEAD, 2 * HEAD), 1)
    is_peak = (src == 64) | (src == 80) | (src == 96)
    is_total = (src == 112) | (src == 120)
    spread = jnp.where(((dst < HEAD) & is_peak) | ((dst >= HEAD) & is_total), 1.0, 0.0).astype(BF16)
    stats = jnp.dot(flat.astype(BF16), spread, preferred_element_type=F32)
    total = stats[:, HEAD:].reshape(n_src, 8, HEAD)
    peak = jnp.where(total > 0.0, stats[:, :HEAD].reshape(n_src, 8, HEAD), NEG_FILL)
    top = jnp.max(peak, axis=0)
    factor = jnp.exp(peak - top[None])
    whole = jnp.sum(factor * total, axis=0)
    mix = jnp.sum(factor * flat.reshape(n_src, 8, HEAD), axis=0)
    attention = mix / jnp.where(whole > 0.0, whole, 1.0)
    attention = jnp.where(iota((8, HEAD), 1) < 64, attention, 0.0)
    both = jnp.concatenate([attention, pltpu.roll(attention, 64, 1)], axis=0).astype(BF16)
    weights = got_ref[:, 0:32, :].reshape(n_src * 32, HEAD)
    result = lax.dot_general(both, weights, NT, preferred_element_type=F32)
    for y in range(out_ref.shape[1]):
        for h in range(2):
            for half in range(2):
                at = (y * 2 + half) * HEAD
                out_ref[:, y, h * 2 + half, :] = result[h * 8 : (h + 1) * 8, at : at + HEAD]


def finish(part_ref, out_ref):
    v = jnp.sum(part_ref[...], axis=0)
    lane = iota((1, HEAD), 1)
    for q in range(4):
        a = v[q // 2 : q // 2 + 1]
        b = v[2 + q // 2 : 3 + q // 2]
        shifts = (0, 32, 32, 64) if q % 2 == 0 else (64, 96, 96, 0)
        moved = [
            x if s == 0 else pltpu.roll(x, s, 1) for x, s in zip((a, b, a, b), shifts)
        ]
        block = jnp.where(
            lane < 32, moved[0], jnp.where(lane < 64, moved[1], jnp.where(lane < 96, moved[2], moved[3]))
        )
        out_ref[:, q * HEAD : (q + 1) * HEAD] = block.astype(BF16)


def on_device(queries, slot_request, key_pages, value_pages, page_owner, page_fill, out_weight, axes):
    z, w, y = axes
    nz, nw, ny = (lax.axis_size(a) for a in axes)
    n_inst = nz * nw
    n_req = 32
    sent = pl.pallas_call(
        prepare,
        out_shape=jax.ShapeDtypeStruct((n_inst, 40, HEAD), BF16),
        in_specs=[SMEM, VMEM, VMEM],
        out_specs=VMEM,
        name="prepare",
    )(slot_request, queries, out_weight)
    got = lax.all_to_all(sent, (z, w), 0, 0, tiled=True)
    parts = pl.pallas_call(
        attend,
        out_shape=jax.ShapeDtypeStruct((n_inst, 8, HEAD), BF16),
        in_specs=[SMEM, SMEM, VMEM, VMEM, VMEM],
        out_specs=VMEM,
        scratch_shapes=[pltpu.VMEM((n_req + 1, 8, HEAD), F32)] * 3,
        name="attend",
    )(page_owner, page_fill, got, key_pages, value_pages)
    parts = lax.all_to_all(parts, (z, w), 0, 0, tiled=True)
    columns = pl.pallas_call(
        project,
        out_shape=jax.ShapeDtypeStruct((nw, ny, 4, HEAD), F32),
        in_specs=[VMEM, VMEM],
        out_specs=VMEM,
        name="project",
    )(parts, got)
    columns = lax.all_to_all(columns.reshape(nw * ny, 4, HEAD), (w, y), 0, 0, tiled=True)
    return pl.pallas_call(
        finish,
        out_shape=jax.ShapeDtypeStruct((1, 4 * HEAD), BF16),
        in_specs=[VMEM],
        out_specs=VMEM,
        name="finish",
    )(columns)


def solution(mesh):
    axes = ("z", "w", "y")
    inst, tp = mesh.devices.shape
    cut = Mesh(mesh.devices.reshape(inst // 8, 8, tp), axes)
    i = axes[:2]
    return jax.shard_map(
        functools.partial(on_device, axes=axes),
        mesh=cut,
        in_specs=(P(i, "y"), P(i), P(i, None, "y"), P(i, None, "y"), P(i), P(i), P("y", i)),
        out_specs=P(i, "y"),
        check_vma=False,
    )
```

```python
import functools

import jax
import jax.numpy as jnp
from jax import lax
from jax.experimental import pallas as pl
from jax.experimental.pallas import tpu as pltpu
from jax.sharding import Mesh, PartitionSpec as P

HEAD = 128
NEG_FILL = -1e30
F32, BF16 = jnp.float32, jnp.bfloat16
NT = (((1,), (1,)), ((), ()))
VMEM = pl.BlockSpec(memory_space=pltpu.VMEM)
SMEM = pl.BlockSpec(memory_space=pltpu.SMEM)


def iota(shape, dim):
    return lax.broadcasted_iota(jnp.int32, shape, dim)


def prepare(req_ref, q_ref, w_ref, out_ref):
    cols, feats = w_ref.shape
    half = cols // 2
    lane = iota((half, HEAD), 1)
    chunks = []
    for m in range(feats // HEAD):
        low = w_ref[:half, m * HEAD : (m + 1) * HEAD].astype(F32)
        high = w_ref[half:, m * HEAD : (m + 1) * HEAD].astype(F32)
        chunks.append(jnp.where(lane < 64, low, pltpu.roll(high, 64, 1)).astype(BF16))
        chunks.append(jnp.where(lane < 64, pltpu.roll(low, 64, 1), high).astype(BF16))
    row = iota((8, HEAD), 0)
    tile = jnp.full((8, HEAD), req_ref[0].astype(F32), F32)
    for h in range(4):
        head = q_ref[:, h * HEAD : (h + 1) * HEAD].astype(F32)
        tile = jnp.where(row == h, jnp.broadcast_to(head, (8, HEAD)), tile)
    tile = tile.astype(BF16)
    for d in range(out_ref.shape[0]):
        out_ref[d, 0:half, :] = chunks[d % len(chunks)]
        out_ref[d, half : half + 8, :] = tile


def three_parts(x):
    hi = x.astype(BF16).astype(F32)
    rest = x - hi
    mid = rest.astype(BF16).astype(F32)
    return hi, mid, rest - mid


def attend(owner_ref, fill_ref, got_ref, k_ref, v_ref, out_ref, peak_ref, mix_ref, sum_ref):
    n_slots = got_ref.shape[0]
    n_pages = k_ref.shape[0]
    n_req = peak_ref.shape[0] - 1
    rows = got_ref[:, 32:40, :].astype(F32).reshape(n_slots * 8, HEAD)
    rows_bf = rows.astype(BF16)
    first = (iota((8, HEAD), 1) == 0).astype(F32).astype(BF16)
    ids = lax.dot_general(first, rows_bf, NT, preferred_element_type=F32)
    blocks = [
        pltpu.roll(ids[:, b * HEAD : (b + 1) * HEAD], HEAD - 4, 1) for b in range(n_slots * 8 // HEAD)
    ]
    here = (iota((8, HEAD), 1) % 8 == iota((8, HEAD), 0)) & (iota((8, HEAD), 0) < 4)
    blocks = [jnp.where(here, b, -5.0) for b in blocks]
    owners = [owner_ref[p] for p in range(n_pages)]
    picks = []
    for p in range(n_pages):
        wanted = jnp.where(owners[p] >= 0, owners[p], -7).astype(F32)
        picks.append(jnp.concatenate([jnp.where(b == wanted, 1.0, 0.0) for b in blocks], axis=1))
    pick = jnp.concatenate(picks, axis=0).astype(BF16)
    page_q = jnp.dot(pick, rows_bf, preferred_element_type=F32)

    peak_ref[...] = jnp.full(peak_ref.shape, NEG_FILL, F32)
    mix_ref[...] = jnp.zeros(mix_ref.shape, F32)
    sum_ref[...] = jnp.zeros(sum_ref.shape, F32)
    token = iota((8, HEAD), 1)
    peaks, totals, outs = [], [], []
    for p in range(n_pages):
        score = lax.dot_general(
            page_q[p * 8 : (p + 1) * 8].astype(BF16), k_ref[p], NT, preferred_element_type=F32
        ) * (HEAD**-0.5)
        score = jnp.where(token < fill_ref[p], score, NEG_FILL)
        peak = jnp.max(score, axis=1, keepdims=True)
        e = jnp.exp(score - peak)
        totals.append(jnp.sum(e, axis=1, keepdims=True))
        outs.append(jnp.dot(e.astype(BF16), v_ref[p], preferred_element_type=F32))
        peaks.append(jnp.broadcast_to(peak, (8, HEAD)))
    index = [jnp.where(o >= 0, o, n_req) for o in owners]
    for p in range(n_pages):
        peak_ref[index[p]] = jnp.maximum(peak_ref[index[p]], peaks[p])
    for p in range(n_pages):
        weight = jnp.exp(peaks[p] - peak_ref[index[p]])
        mix_ref[index[p]] += weight * outs[p]
        sum_ref[index[p]] += weight * totals[p]

    n_rows = n_req * 8
    lane = iota((n_rows, HEAD), 1)
    mix = mix_ref[0:n_req].reshape(n_rows, HEAD)
    total = sum_ref[0:n_req].reshape(n_rows, HEAD)
    hi, mid, low = three_parts(peak_ref[0:n_req].reshape(n_rows, HEAD))
    total_hi = total.astype(BF16).astype(F32)
    stats = jnp.where(
        lane < 80,
        hi,
        jnp.where(lane < 96, mid, jnp.where(lane < 112, low, jnp.where(lane < 120, total_hi, total - total_hi))),
    )
    data = jnp.concatenate([mix.astype(BF16), stats.astype(BF16)], axis=1)
    place = (iota((n_slots, n_slots * 8), 1) == iota((n_slots, n_slots * 8), 0) * 8 + 4)
    slot_id = jnp.dot(place.astype(F32).astype(BF16), rows_bf, preferred_element_type=F32)[:, 0:1]
    col = iota((n_slots, n_rows), 1)
    owns = slot_id == (col // 8).astype(F32)
    lane8 = iota((n_slots, HEAD), 1)
    for h in range(4):
        chosen = jnp.where(owns & (col % 8 == h), 1.0, 0.0).astype(BF16)
        picked = jnp.dot(chosen, data, preferred_element_type=F32)
        o, st = picked[:, :HEAD], picked[:, HEAD:]
        left = jnp.where(lane8 < 64, o, st)
        right = jnp.where(lane8 < 64, pltpu.roll(o, 64, 1), st)
        for z in range(n_slots // 8):
            out_ref[z * 8 + 2 * h] = left[z * 8 : (z + 1) * 8].astype(BF16)
            out_ref[z * 8 + 2 * h + 1] = right[z * 8 : (z + 1) * 8].astype(BF16)


def project(part_ref, got_ref, out_ref):
    n_src = part_ref.shape[0]
    flat = part_ref[...].astype(F32).reshape(n_src * 8, HEAD)
    src = iota((HEAD, 2 * HEAD), 0)
    dst = iota((HEAD, 2 * HEAD), 1)
    is_peak = (src == 64) | (src == 80) | (src == 96)
    is_total = (src == 112) | (src == 120)
    spread = jnp.where(((dst < HEAD) & is_peak) | ((dst >= HEAD) & is_total), 1.0, 0.0).astype(BF16)
    stats = jnp.dot(flat.astype(BF16), spread, preferred_element_type=F32)
    total = stats[:, HEAD:].reshape(n_src, 8, HEAD)
    peak = jnp.where(total > 0.0, stats[:, :HEAD].reshape(n_src, 8, HEAD), NEG_FILL)
    top = jnp.max(peak, axis=0)
    factor = jnp.exp(peak - top[None])
    whole = jnp.sum(factor * total, axis=0)
    mix = jnp.sum(factor * flat.reshape(n_src, 8, HEAD), axis=0)
    attention = mix / jnp.where(whole > 0.0, whole, 1.0)
    attention = jnp.where(iota((8, HEAD), 1) < 64, attention, 0.0)
    both = jnp.concatenate([attention, pltpu.roll(attention, 64, 1)], axis=0).astype(BF16)
    weights = got_ref[:, 0:32, :].reshape(n_src * 32, HEAD)
    result = lax.dot_general(both, weights, NT, preferred_element_type=F32)
    for y in range(out_ref.shape[1]):
        for h in range(2):
            for half in range(2):
                at = (y * 2 + half) * HEAD
                out_ref[:, y, h * 2 + half, :] = result[h * 8 : (h + 1) * 8, at : at + HEAD]


def finish(part_ref, out_ref):
    v = jnp.sum(part_ref[...], axis=0)
    lane = iota((1, HEAD), 1)
    for q in range(4):
        a = v[q // 2 : q // 2 + 1]
        b = v[2 + q // 2 : 3 + q // 2]
        shifts = (0, 32, 32, 64) if q % 2 == 0 else (64, 96, 96, 0)
        moved = [
            x if s == 0 else pltpu.roll(x, s, 1) for x, s in zip((a, b, a, b), shifts)
        ]
        block = jnp.where(
            lane < 32, moved[0], jnp.where(lane < 64, moved[1], jnp.where(lane < 96, moved[2], moved[3]))
        )
        out_ref[:, q * HEAD : (q + 1) * HEAD] = block.astype(BF16)


def on_device(queries, slot_request, key_pages, value_pages, page_owner, page_fill, out_weight, axes):
    z, w, y = axes
    nz, nw, ny = (lax.axis_size(a) for a in axes)
    n_inst = nz * nw
    n_req = 32
    limit = pltpu.CompilerParams(vmem_limit_bytes=12 << 20)
    sent = pl.pallas_call(
        prepare,
        out_shape=jax.ShapeDtypeStruct((n_inst, 40, HEAD), BF16),
        in_specs=[SMEM, VMEM, VMEM],
        out_specs=VMEM,
        compiler_params=limit,
        name="prepare",
    )(slot_request, queries, out_weight.T)
    got = lax.all_to_all(sent, (z, w), 0, 0, tiled=True)
    parts = pl.pallas_call(
        attend,
        out_shape=jax.ShapeDtypeStruct((n_inst, 8, HEAD), BF16),
        in_specs=[SMEM, SMEM, VMEM, VMEM, VMEM],
        out_specs=VMEM,
        scratch_shapes=[pltpu.VMEM((n_req + 1, 8, HEAD), F32)] * 3,
        compiler_params=limit,
        name="attend",
    )(page_owner, page_fill, got, key_pages, value_pages)
    parts = lax.all_to_all(parts, (z, w), 0, 0, tiled=True)
    columns = pl.pallas_call(
        project,
        out_shape=jax.ShapeDtypeStruct((nw, ny, 4, HEAD), F32),
        in_specs=[VMEM, VMEM],
        out_specs=VMEM,
        compiler_params=limit,
        name="project",
    )(parts, got)
    columns = lax.all_to_all(columns.reshape(nw * ny, 4, HEAD), (w, y), 0, 0, tiled=True)
    return pl.pallas_call(
        finish,
        out_shape=jax.ShapeDtypeStruct((1, 4 * HEAD), BF16),
        in_specs=[VMEM],
        out_specs=VMEM,
        compiler_params=limit,
        name="finish",
    )(columns)


def solution(mesh):
    axes = ("z", "w", "y")
    inst, tp = mesh.devices.shape
    cut = Mesh(mesh.devices.reshape(inst // 8, 8, tp), axes)
    i = axes[:2]
    return jax.shard_map(
        functools.partial(on_device, axes=axes),
        mesh=cut,
        in_specs=(P(i, "y"), P(i), P(i, None, "y"), P(i, None, "y"), P(i), P(i), P("y", i)),
        out_specs=P(i, "y"),
        check_vma=False,
    )
```

```python
import functools

import jax
import jax.numpy as jnp
from jax import lax
from jax.experimental import pallas as pl
from jax.experimental.pallas import tpu as pltpu
from jax.sharding import Mesh, PartitionSpec as P

HEAD = 128
NEG_FILL = -1e30
F32, BF16 = jnp.float32, jnp.bfloat16
NT = (((1,), (1,)), ((), ()))
VMEM = pl.BlockSpec(memory_space=pltpu.VMEM)
SMEM = pl.BlockSpec(memory_space=pltpu.SMEM)
HBM = pl.BlockSpec(memory_space=pltpu.HBM)


def iota(shape, dim):
    return lax.broadcasted_iota(jnp.int32, shape, dim)


def prepare(req_ref, q_hbm, w_hbm, v_hbm, out_ref, v_ref, q_ref, w_ref, sems):
    pairs = ((q_hbm, q_ref), (w_hbm, w_ref), (v_hbm, v_ref))
    copies = [pltpu.make_async_copy(a, b, sems.at[n]) for n, (a, b) in enumerate(pairs)]
    for copy in copies:
        copy.start()
    for copy in copies[:2]:
        copy.wait()
    cols, feats = w_ref.shape
    half = cols // 2
    lane = iota((half, HEAD), 1)
    chunks = []
    for m in range(feats // HEAD):
        low = w_ref[:half, m * HEAD : (m + 1) * HEAD].astype(F32)
        high = w_ref[half:, m * HEAD : (m + 1) * HEAD].astype(F32)
        chunks.append(jnp.where(lane < 64, low, pltpu.roll(high, 64, 1)).astype(BF16))
        chunks.append(jnp.where(lane < 64, pltpu.roll(low, 64, 1), high).astype(BF16))
    row = iota((8, HEAD), 0)
    tile = jnp.full((8, HEAD), req_ref[0].astype(F32), F32)
    for h in range(4):
        head = q_ref[:, h * HEAD : (h + 1) * HEAD].astype(F32)
        tile = jnp.where(row == h, jnp.broadcast_to(head, (8, HEAD)), tile)
    tile = tile.astype(BF16)
    for d in range(out_ref.shape[0]):
        out_ref[d, 0:half, :] = chunks[d % len(chunks)]
        out_ref[d, half : half + 8, :] = tile
    copies[2].wait()


def keep(x):
    return pltpu.with_memory_space_constraint(x, pltpu.HBM)


def three_parts(x):
    hi = x.astype(BF16).astype(F32)
    rest = x - hi
    mid = rest.astype(BF16).astype(F32)
    return hi, mid, rest - mid


def attend(owner_ref, fill_ref, got_ref, k_ref, v_ref, out_ref, peak_ref, mix_ref, sum_ref):
    n_slots = got_ref.shape[0]
    n_pages = k_ref.shape[0]
    n_pairs = n_pages // 2
    n_req = peak_ref.shape[0] - 1
    row8 = iota((8, HEAD), 0)
    lane = iota((8, HEAD), 1)
    first = row8 < 4
    rows_bf = got_ref[:, 32:40, :].astype(F32).reshape(n_slots * 8, HEAD).astype(BF16)
    unit = (lane == 0).astype(F32).astype(BF16)
    ids = lax.dot_general(unit, rows_bf, NT, preferred_element_type=F32)
    here = (lane % 8) == (row8 % 4)
    blocks = [
        jnp.where(here, pltpu.roll(ids[:, b * HEAD : (b + 1) * HEAD], HEAD - 4, 1), -5.0)
        for b in range(n_slots * 8 // HEAD)
    ]
    owners = [owner_ref[p] for p in range(n_pages)]
    picks = []
    for i in range(n_pairs):
        a, b = owners[2 * i], owners[2 * i + 1]
        wanted = jnp.where(first, jnp.where(a >= 0, a, -7), jnp.where(b >= 0, b, -7)).astype(F32)
        picks.append(jnp.concatenate([jnp.where(x == wanted, 1.0, 0.0) for x in blocks], axis=1))
    pick = jnp.concatenate(picks, axis=0).astype(BF16)
    page_q = jnp.dot(pick, rows_bf, preferred_element_type=F32)
    scores = []
    for i in range(n_pairs):
        pair = k_ref[2 * i : 2 * i + 2].reshape(2 * HEAD, HEAD)
        s = lax.dot_general(page_q[8 * i : 8 * i + 8].astype(BF16), pair, NT, preferred_element_type=F32)
        s = jnp.where(first, s[:, :HEAD], s[:, HEAD:])
        fill = jnp.where(first, fill_ref[2 * i], fill_ref[2 * i + 1])
        scores.append(jnp.where(lane < fill, s * (HEAD**-0.5), NEG_FILL))
    score = jnp.concatenate(scores, axis=0)
    peak = jnp.broadcast_to(jnp.max(score, axis=1, keepdims=True), score.shape)
    e = jnp.exp(score - peak)
    total = jnp.broadcast_to(jnp.sum(e, axis=1, keepdims=True), score.shape)
    low = (iota(e.shape, 0) % 8) < 4
    spread = jnp.concatenate([jnp.where(low, e, 0.0), jnp.where(low, 0.0, e)], axis=1)
    outs = []
    for i in range(n_pairs):
        pair = v_ref[2 * i : 2 * i + 2].reshape(2 * HEAD, HEAD)
        outs.append(jnp.dot(spread[8 * i : 8 * i + 8].astype(BF16), pair, preferred_element_type=F32))
    peak_ref[...] = jnp.full(peak_ref.shape, NEG_FILL, F32)
    mix_ref[...] = jnp.zeros(mix_ref.shape, F32)
    sum_ref[...] = jnp.zeros(sum_ref.shape, F32)
    index = [jnp.where(o >= 0, o, n_req) for o in owners]
    for p in range(n_pages):
        mine = first if p % 2 == 0 else jnp.logical_not(first)
        at = 8 * (p // 2)
        peak_ref[index[p]] = jnp.maximum(peak_ref[index[p]], jnp.where(mine, peak[at : at + 8], NEG_FILL))
    every = peak_ref[...]
    peak_ref[...] = jnp.maximum(every, pltpu.roll(every, 4, 1))
    for p in range(n_pages):
        mine = first if p % 2 == 0 else jnp.logical_not(first)
        at = 8 * (p // 2)
        weight = jnp.where(mine, jnp.exp(peak[at : at + 8] - peak_ref[index[p]]), 0.0)
        mix_ref[index[p]] += weight * outs[p // 2]
        sum_ref[index[p]] += weight * total[at : at + 8]
    n_rows = n_req * 8
    mix = mix_ref[0:n_req]
    mix = (mix + pltpu.roll(mix, 4, 1)).reshape(n_rows, HEAD)
    total = sum_ref[0:n_req]
    total = (total + pltpu.roll(total, 4, 1)).reshape(n_rows, HEAD)
    lane_n = iota((n_rows, HEAD), 1)
    hi, mid, rest = three_parts(peak_ref[0:n_req].reshape(n_rows, HEAD))
    total_hi = total.astype(BF16).astype(F32)
    stats = jnp.where(lane_n < 80, hi, jnp.where(lane_n < 96, mid, jnp.where(lane_n < 112, rest, jnp.where(lane_n < 120, total_hi, total - total_hi))))
    data = jnp.concatenate([mix.astype(BF16), stats.astype(BF16)], axis=1)
    place = iota((n_slots, n_slots * 8), 1) == iota((n_slots, n_slots * 8), 0) * 8 + 4
    slot_id = jnp.dot(place.astype(F32).astype(BF16), rows_bf, preferred_element_type=F32)
    slot_id = jnp.concatenate([slot_id, slot_id], axis=1)
    col = iota((n_slots, n_rows), 1)
    owns = slot_id == (col // 8).astype(F32)
    left64 = iota((n_slots, HEAD), 1) < 64
    for h in range(4):
        chosen = jnp.where(owns & (col % 8 == h), 1.0, 0.0).astype(BF16)
        picked = jnp.dot(chosen, data, preferred_element_type=F32)
        o, st = picked[:, :HEAD], picked[:, HEAD:]
        left = jnp.where(left64, o, st)
        right = jnp.where(left64, pltpu.roll(o, 64, 1), st)
        for z in range(n_slots // 8):
            out_ref[z * 8 + 2 * h] = left[z * 8 : (z + 1) * 8].astype(BF16)
            out_ref[z * 8 + 2 * h + 1] = right[z * 8 : (z + 1) * 8].astype(BF16)


def project(part_ref, got_ref, out_ref):
    n_src = part_ref.shape[0]
    flat = part_ref[...].astype(F32).reshape(n_src * 8, HEAD)
    src = iota((HEAD, 2 * HEAD), 0)
    dst = iota((HEAD, 2 * HEAD), 1)
    is_peak = (src == 64) | (src == 80) | (src == 96)
    is_total = (src == 112) | (src == 120)
    spread = jnp.where(((dst < HEAD) & is_peak) | ((dst >= HEAD) & is_total), 1.0, 0.0).astype(BF16)
    stats = jnp.dot(flat.astype(BF16), spread, preferred_element_type=F32)
    total = stats[:, HEAD:].reshape(n_src, 8, HEAD)
    peak = jnp.where(total > 0.0, stats[:, :HEAD].reshape(n_src, 8, HEAD), NEG_FILL)
    top = jnp.max(peak, axis=0)
    factor = jnp.exp(peak - top[None])
    whole = jnp.sum(factor * total, axis=0)
    mix = jnp.sum(factor * flat.reshape(n_src, 8, HEAD), axis=0)
    attention = mix / jnp.where(whole > 0.0, whole, 1.0)
    attention = jnp.where(iota((8, HEAD), 1) < 64, attention, 0.0)
    both = jnp.concatenate([attention, pltpu.roll(attention, 64, 1)], axis=0).astype(BF16)
    weights = got_ref[:, 0:32, :].reshape(n_src * 32, HEAD)
    result = lax.dot_general(both, weights, NT, preferred_element_type=F32)
    for y in range(out_ref.shape[1]):
        for h in range(2):
            for half in range(2):
                at = (y * 2 + half) * HEAD
                out_ref[:, y, h * 2 + half, :] = result[h * 8 : (h + 1) * 8, at : at + HEAD]


def finish(part_ref, out_ref):
    v = jnp.sum(part_ref[...], axis=0)
    lane = iota((1, HEAD), 1)
    for q in range(4):
        a = v[q // 2 : q // 2 + 1]
        b = v[2 + q // 2 : 3 + q // 2]
        shifts = (0, 32, 32, 64) if q % 2 == 0 else (64, 96, 96, 0)
        moved = [
            x if s == 0 else pltpu.roll(x, s, 1) for x, s in zip((a, b, a, b), shifts)
        ]
        block = jnp.where(
            lane < 32, moved[0], jnp.where(lane < 64, moved[1], jnp.where(lane < 96, moved[2], moved[3]))
        )
        out_ref[:, q * HEAD : (q + 1) * HEAD] = block.astype(BF16)


def on_device(queries, slot_request, key_pages, value_pages, page_owner, page_fill, out_weight, axes):
    z, w, y = axes
    nz, nw, ny = (lax.axis_size(a) for a in axes)
    n_inst = nz * nw
    n_req = 32
    limit = pltpu.CompilerParams(vmem_limit_bytes=12 << 20)
    sent, values = pl.pallas_call(
        prepare,
        out_shape=[jax.ShapeDtypeStruct((n_inst, 40, HEAD), BF16), jax.ShapeDtypeStruct(value_pages.shape, BF16)],
        in_specs=[SMEM, HBM, HBM, HBM],
        out_specs=[VMEM, VMEM],
        scratch_shapes=[
            pltpu.VMEM(queries.shape, BF16),
            pltpu.VMEM(out_weight.shape[::-1], BF16),
            pltpu.SemaphoreType.DMA((3,)),
        ],
        compiler_params=limit,
        name="prepare",
    )(slot_request, keep(queries), keep(out_weight.T), keep(value_pages))
    got = lax.all_to_all(sent, (z, w), 0, 0, tiled=True)
    parts = pl.pallas_call(
        attend,
        out_shape=jax.ShapeDtypeStruct((n_inst, 8, HEAD), BF16),
        in_specs=[SMEM, SMEM, VMEM, VMEM, VMEM],
        out_specs=VMEM,
        scratch_shapes=[pltpu.VMEM((n_req + 1, 8, HEAD), F32)] * 3,
        compiler_params=limit,
        name="attend",
    )(page_owner, page_fill, got, key_pages, values)
    parts = lax.all_to_all(parts, (z, w), 0, 0, tiled=True)
    columns = pl.pallas_call(
        project,
        out_shape=jax.ShapeDtypeStruct((nw, ny, 4, HEAD), F32),
        in_specs=[VMEM, VMEM],
        out_specs=VMEM,
        compiler_params=limit,
        name="project",
    )(parts, got)
    columns = lax.all_to_all(columns.reshape(nw * ny, 4, HEAD), (w, y), 0, 0, tiled=True)
    return pl.pallas_call(
        finish,
        out_shape=jax.ShapeDtypeStruct((1, 4 * HEAD), BF16),
        in_specs=[VMEM],
        out_specs=VMEM,
        compiler_params=limit,
        name="finish",
    )(columns)


def solution(mesh):
    axes = ("z", "w", "y")
    inst, tp = mesh.devices.shape
    cut = Mesh(mesh.devices.reshape(inst // 8, 8, tp), axes)
    i = axes[:2]
    return jax.shard_map(
        functools.partial(on_device, axes=axes),
        mesh=cut,
        in_specs=(P(i, "y"), P(i), P(i, None, "y"), P(i, None, "y"), P(i), P(i), P("y", i)),
        out_specs=P(i, "y"),
        check_vma=False,
    )
```
